32 devices in a mesh: rows: 8 (over z, y), feat: 4 (over x, core).
Axes of the slice: x: 2, y: 2, z: 4, core: 2. Of those that a mesh axis runs over, the one named last changes fastest.
Arguments:
- bin_index: int32 [16384, 512], P('rows', 'feat'), may hold values from 0 to 255
- leaf_ids: int32 [16384], P('rows'), may hold values from 0 to 15
- gradients: bfloat16 [16384], P('rows'), may hold values from -3 to 3
- hessians: bfloat16 [16384], P('rows'), may hold values from 0.049804688 to 0.25
Outputs:
- split_gains: float32 [4, 128, 16, 256], P('feat', 'rows')
- best_gain: float32 [16], replicated
The draws below stay inside these ranges and needn't reach their ends.
All inputs are finite; a program needn't handle non-finite values.
Results may differ from the reference program's by a relative error of at most 0.0003.
Values may be sent and summed in bfloat16 or wider, within the bound.
A program may use at most 64 MiB of HBM per device.

```python
import math
import jax
import jax.numpy as jnp
import numpy as np
from jax import lax

FEATURES = 512
BINS = 256
LEAVES = 16
ROW_TOTAL = 16384
N_FEAT = 4


def touch_ends(entries, rng, low, high):
    longest = entries.shape.index(max(entries.shape))
    spots = []
    for shift in (0, 1):
        where = [jax.random.randint(jax.random.fold_in(rng, axis), (), 0, length) for axis, length in enumerate(entries.shape)]
        where[longest] = (where[longest] + shift) % entries.shape[longest]
        spots.append(tuple(where))
    return entries.at[spots[0]].set(low).at[spots[1]].set(high)


def block_levels(key, extent, cuts, low, top_value):
    factor_of, own = 1.0, jax.random.fold_in(key, 6)
    for position, shards_of in cuts:
        steps = jnp.exp(jax.random.uniform(jax.random.fold_in(own, position), (shards_of,), jnp.float32, low / len(cuts), top_value / len(cuts)))
        factor_of = factor_of * jnp.repeat(steps, extent[position] // shards_of).reshape([-1 if axis == position else 1 for axis in range(len(extent))])
    return factor_of


def cumulative_ranks(number_of, lean):
    loads = [(1 << 20) // math.isqrt(standing ** lean) + 1 for standing in range(1, number_of + 1)]
    width = 1 + sum(loads) // (1 << 30)
    return np.cumsum(np.array([max(1, weight // width) for weight in loads]))


def skewed_ids(own_key, shape, amount, lean):
    grid = cumulative_ranks(amount, lean)
    pick = jax.random.randint(jax.random.fold_in(own_key, 1), shape, 0, int(grid[amount - 1]))
    standing = jnp.searchsorted(jnp.asarray(grid, jnp.int32), pick, side="right")
    return jax.random.permutation(jax.random.fold_in(own_key, 2), amount)[standing].astype(jnp.int32)


def noise(stream_key, shape, spread, most, split=(), kind=jnp.bfloat16):
    loudness = block_levels(stream_key, shape, split, -0.22, 0.18) if split else 1.0
    result = jax.random.normal(stream_key, shape, jnp.float32) * spread * loudness
    return jnp.minimum(jnp.maximum(result, -most), most).astype(kind)


def setup_inputs(seed: int = 0) -> dict:
    arg_keys = jax.random.split(jax.random.key(seed), 5)
    return {
        "bin_index": touch_ends(jax.random.randint(arg_keys[0], (ROW_TOTAL, FEATURES), 0, BINS), jax.random.fold_in(arg_keys[0], 1), 0, BINS - 1).astype(jnp.int32),
        "leaf_ids": touch_ends(skewed_ids(arg_keys[1], (ROW_TOTAL,), LEAVES, 2), jax.random.fold_in(arg_keys[1], 3), 0, LEAVES - 1).astype(jnp.int32),
        "gradients": noise(arg_keys[2], (ROW_TOTAL,), 0.5, 3.0, ((0, 8),)),
        "hessians": jnp.clip(jnp.exp(math.log(0.25) - 1.6133518 * jax.random.uniform(arg_keys[3], (ROW_TOTAL,), jnp.float32) ** block_levels(arg_keys[3], (ROW_TOTAL,), ((0, 8),), -0.2, 0.2)), 0.049804688, 0.25).astype(jnp.bfloat16),
    }


reg_lambda = 1.0


def gain_of(left_grad, left_hess):
    total_grad = left_grad[:, :, -1:]
    total_hess = left_hess[:, :, -1:]
    right_grad = total_grad - left_grad
    right_hess = total_hess - left_hess
    return 0.5 * (left_grad * left_grad / (left_hess + reg_lambda)
                  + right_grad * right_grad / (right_hess + reg_lambda)
                  - total_grad * total_grad / (total_hess + reg_lambda))


def reference(bin_index, leaf_ids, gradients, hessians):
    grad_wide = gradients.astype(jnp.float32)
    hess_wide = hessians.astype(jnp.float32)
    group_width = math.gcd(FEATURES, 16)
    block_count = FEATURES // group_width
    segment_total = group_width * LEAVES * BINS

    def one_block(columns):
        offsets = jnp.arange(group_width, dtype=jnp.int32) * (LEAVES * BINS)
        flat_index = offsets[None, :] + leaf_ids[:, None] * BINS + columns
        flat_index = flat_index.reshape(-1)
        grad_flat = jnp.broadcast_to(grad_wide[:, None], columns.shape).reshape(-1)
        hess_flat = jnp.broadcast_to(hess_wide[:, None], columns.shape).reshape(-1)
        grad_hist = jax.ops.segment_sum(grad_flat, flat_index, num_segments=segment_total)
        hess_hist = jax.ops.segment_sum(hess_flat, flat_index, num_segments=segment_total)
        return (grad_hist.reshape(group_width, LEAVES, BINS), hess_hist.reshape(group_width, LEAVES, BINS))

    blocked = bin_index.reshape(ROW_TOTAL, block_count, group_width).transpose(1, 0, 2)
    hist_grad, hist_hess = lax.map(one_block, blocked)
    hist_grad = hist_grad.reshape(FEATURES, LEAVES, BINS)
    hist_hess = hist_hess.reshape(FEATURES, LEAVES, BINS)
    left_grad = jnp.cumsum(hist_grad, axis=2)
    left_hess = jnp.cumsum(hist_hess, axis=2)
    split_gains = gain_of(left_grad, left_hess)
    best_gain = jnp.max(split_gains, axis=(0, 2))
    return split_gains.reshape(N_FEAT, FEATURES // N_FEAT, LEAVES, BINS), best_gain
```

```python
import functools

import jax
import jax.numpy as jnp
from jax import lax
from jax.experimental import pallas as pl
from jax.experimental.pallas import tpu as pltpu
from jax.sharding import PartitionSpec as P

BINS = 256
LEAVES = 16
LANES = 128
HALF = BINS // 2
MESH = pl.DeviceIdType.MESH

reg_lambda = 1.0


def kernel(n, n_feat, group, bins_hbm, leaf_hbm, grad_hbm, hess_hbm, gain_ref, best_ref,
           leaf_ref, grad_ref, hess_ref, small_sems, raw, bins_src, meta_src, columns, metas, weights, sums, top, landing,
           raw_sems, bin_send, bin_recv, meta_send, meta_recv, swap_send, swap_recv, own_sems, top_send, top_recv):
    me, me_feat = lax.axis_index("rows"), lax.axis_index("feat")
    everyone = n * n_feat
    me_all = me * n_feat + me_feat
    own, rows = bins_src.shape[1], bins_src.shape[2]
    tiles = rows // LANES
    share = tiles // n_feat
    half = n // 2
    across = (1 - me // half) * half
    pieces = raw_sems.shape[0]
    piece_rows = rows // pieces

    def fetch(piece):
        span = pl.ds(piece * piece_rows, piece_rows)
        return pltpu.make_async_copy(bins_hbm.at[span], raw.at[span], raw_sems.at[piece])

    small = [pltpu.make_async_copy(source, target, small_sems.at[place]) for place, (source, target) in enumerate(
        ((leaf_hbm, leaf_ref), (grad_hbm, grad_ref), (hess_hbm, hess_ref)))]
    for copy in small:
        copy.start()
    for piece in range(pieces):
        fetch(piece).start()

    def partner(step):
        other, bit = 0, 1
        while bit < n:
            other += lax.rem(me // bit + step // bit, 2) * bit
            bit *= 2
        return other

    def device_after(step):
        return {"rows": partner(step // n_feat), "feat": lax.rem(me_feat + lax.rem(step, n_feat), n_feat)}

    barrier = pltpu.get_barrier_semaphore()

    def each(first, last, act):
        def run(step, carry):
            act(step)
            return carry
        lax.fori_loop(first, last, run, 0, unroll=everyone <= 64)

    def greet(device):
        pl.semaphore_signal(barrier, inc=1, device_id=device, device_id_type=MESH)

    each(1, n, lambda step: greet({"rows": partner(n - step)}))
    each(1, n_feat, lambda step: greet(device_after(step)))

    for copy in small:
        copy.wait()
    leaf, grad, hess = (ref[...].astype(jnp.float32) for ref in (leaf_ref, grad_ref, hess_ref))
    spare = jnp.zeros((meta_src.shape[1] - 3 * share, LANES), jnp.float32)
    for part in range(n_feat):
        span = slice(part * share, (part + 1) * share)
        meta_src[part] = jnp.concatenate([leaf[span], grad[span], hess[span], spare], axis=0).astype(jnp.bfloat16)
    for piece in range(pieces):
        fetch(piece).wait()
        for tile in range(piece * piece_rows // LANES, (piece + 1) * piece_rows // LANES):
            lanes = slice(tile * LANES, (tile + 1) * LANES)
            turned = raw[lanes].astype(jnp.float32).T.astype(jnp.bfloat16)
            bins_src[:, :, lanes] = turned.reshape(n, own, LANES)

    own_bins = pltpu.make_async_copy(bins_src.at[me], columns.at[me], own_sems.at[0])
    own_meta = pltpu.make_async_copy(meta_src, metas.at[:, me], own_sems.at[1])
    own_bins.start()
    own_meta.start()
    pl.semaphore_wait(barrier, n - 1 + n_feat - 1)

    def bin_copy(step, landed):
        other = partner(step)
        return pltpu.make_async_remote_copy(
            src_ref=bins_src.at[other], dst_ref=columns.at[other if landed else me], send_sem=bin_send.at[step],
            recv_sem=bin_recv.at[step], device_id={"rows": other}, device_id_type=MESH)

    def near_meta(step, landed):
        other = partner(step)
        return pltpu.make_async_remote_copy(
            src_ref=meta_src, dst_ref=metas.at[:, other if landed else me], send_sem=meta_send.at[step],
            recv_sem=meta_recv.at[step], device_id={"rows": other}, device_id_type=MESH)

    def far_meta(step, landed):
        other = partner(step)
        return pltpu.make_async_remote_copy(
            src_ref=meta_src.at[me_feat], dst_ref=metas.at[me_feat, other if landed else me], send_sem=meta_send.at[step],
            recv_sem=meta_recv.at[step], device_id={"rows": other}, device_id_type=MESH)

    def swap_meta(step, landed):
        held = lax.rem(me_feat + n_feat - step, n_feat) if landed else me_feat
        far = metas.at[held, pl.ds(across, half)]
        return pltpu.make_async_remote_copy(
            src_ref=far, dst_ref=far, send_sem=swap_send.at[step], recv_sem=swap_recv.at[step],
            device_id={"feat": lax.rem(me_feat + step, n_feat)}, device_id_type=MESH)

    each(half, n, lambda step: far_meta(step, False).start())
    each(1, half, lambda step: near_meta(step, False).start())
    each(1, n, lambda step: bin_copy(step, False).start())
    sums[...] = jnp.zeros_like(sums)
    landing[0] = jnp.full((1, LANES), -jnp.inf, jnp.float32)
    own_bins.wait()
    own_meta.wait()

    def one_shard(step, carry):
        origin = partner(step)

        @pl.when(step == min(2, half - 1))
        def swap():
            each(half, n, lambda far: far_meta(far, True).wait_recv())
            each(1, n_feat, lambda other: swap_meta(other, False).start())

        @pl.when(jnp.logical_and(step > 0, step < half))
        def near_arrived():
            near_meta(step, True).wait_recv()

        @pl.when(step == half)
        def swapped():
            each(1, n_feat, lambda other: swap_meta(other, True).wait_recv())

        @pl.when(step > 0)
        def arrived():
            bin_copy(step, True).wait_recv()

        table = metas[:, origin].astype(jnp.float32)
        leaf_of = lax.broadcasted_iota(jnp.int32, (LEAVES, LANES), 0).astype(jnp.float32)
        for tile in range(tiles):
            piece, row = tile // share, tile % share
            member = jnp.broadcast_to(table[piece, row:row + 1], (LEAVES, LANES)) == leaf_of
            for part in (0, 1):
                first = (1 + part) * share + row
                value = jnp.broadcast_to(table[piece, first:first + 1], (LEAVES, LANES))
                weights[part * LEAVES:(part + 1) * LEAVES, tile * LANES:(tile + 1) * LANES] = (
                    jnp.where(member, value, 0.0).astype(jnp.bfloat16))

        block = columns[origin]
        level = lax.broadcasted_iota(jnp.int32, (HALF, rows), 0).astype(jnp.bfloat16)
        one, zero = jnp.ones((), jnp.bfloat16), jnp.zeros((), jnp.bfloat16)
        table_rows = weights[...]
        for first in range(0, own, group):
            left_side, right_side = [], []
            for feature in range(first, first + group):
                bins = block[feature:feature + 1]
                upper = bins >= HALF
                low = jnp.where(upper, bins - HALF, bins)
                upper_wide = jnp.broadcast_to(bins, (2 * LEAVES, rows)) >= HALF
                left_side.append(jnp.where(upper_wide, zero, table_rows))
                left_side.append(jnp.where(upper_wide, table_rows, zero))
                right_side.append(jnp.where(jnp.broadcast_to(low, (HALF, rows)) <= level, one, zero).astype(jnp.float8_e4m3fn))
            product = lax.dot_general(
                jnp.concatenate(left_side, axis=0), jnp.concatenate(right_side, axis=0),
                (((1,), (1,)), ((), ())), preferred_element_type=jnp.float32)
            for place in range(group):
                sums[first + place] += product[place * 4 * LEAVES:(place + 1) * 4 * LEAVES, place * HALF:(place + 1) * HALF]
        return carry

    lax.fori_loop(0, n, one_shard, 0)

    def gains(feature, largest):
        part = sums[feature]
        grad_low, hess_low = part[:LEAVES], part[LEAVES:2 * LEAVES]
        grad_high = part[2 * LEAVES:3 * LEAVES] + grad_low[:, HALF - 1:]
        hess_high = part[3 * LEAVES:] + hess_low[:, HALF - 1:]
        total_grad, total_hess = grad_high[:, HALF - 1:], hess_high[:, HALF - 1:]
        whole = total_grad * total_grad / (total_hess + reg_lambda)
        for place, left_grad, left_hess in ((0, grad_low, hess_low), (1, grad_high, hess_high)):
            right_grad, right_hess = total_grad - left_grad, total_hess - left_hess
            gain = 0.5 * (left_grad * left_grad / (left_hess + reg_lambda)
                          + right_grad * right_grad / (right_hess + reg_lambda) - whole)
            gain_ref[feature, :, place * HALF:(place + 1) * HALF] = gain
            largest = jnp.maximum(largest, gain)
        return largest

    largest = lax.fori_loop(0, own, gains, jnp.full((LEAVES, HALF), -jnp.inf, jnp.float32), unroll=True)
    largest = jnp.broadcast_to(jnp.max(largest, axis=1, keepdims=True), (LEAVES, LANES))
    on_lane = (lax.broadcasted_iota(jnp.int32, (LEAVES, LANES), 0) == lax.broadcasted_iota(jnp.int32, (LEAVES, LANES), 1))
    top[...] = jnp.max(jnp.where(on_lane, largest, -jnp.inf), axis=0, keepdims=True)

    def report(place):
        step = everyone - place
        return pltpu.make_async_remote_copy(
            src_ref=top, dst_ref=landing.at[step], send_sem=top_send.at[step],
            recv_sem=top_recv.at[step], device_id=device_after(step), device_id_type=MESH)

    each(1, everyone, lambda place: report(place).start())
    each(1, n, lambda step: bin_copy(step, False).wait_send())
    each(1, half, lambda step: near_meta(step, False).wait_send())
    each(half, n, lambda step: far_meta(step, False).wait_send())
    each(1, n_feat, lambda step: swap_meta(step, False).wait_send())
    each(1, everyone, lambda place: report(everyone - place).wait_recv())
    best = jnp.maximum(top[...], jnp.max(landing[...], axis=0))
    each(1, everyone, lambda step: report(step).wait_send())
    best_ref[...] = best[:, :LEAVES]


def body(bin_index, leaf_ids, gradients, hessians):
    n, n_feat = lax.axis_size("rows"), lax.axis_size("feat")
    rows, local_features = bin_index.shape
    own = local_features // n
    group = 2 if own % 2 == 0 else 1
    tiles = rows // LANES
    pieces = 4
    everyone = n * n_feat
    meta_rows = -(-3 * (tiles // n_feat) // 16) * 16
    vmem = pl.BlockSpec(memory_space=pltpu.VMEM)
    dma = pltpu.SemaphoreType.DMA
    gain, best = pl.pallas_call(
        functools.partial(kernel, n, n_feat, group),
        out_shape=(pltpu.VMEM((own, LEAVES, BINS), jnp.float32),
                   pltpu.VMEM((1, LEAVES), jnp.float32)),
        in_specs=[pl.BlockSpec(memory_space=pl.ANY)] * 4,
        out_specs=(vmem, vmem),
        scratch_shapes=[
            pltpu.VMEM((tiles, LANES), jnp.int32),
            pltpu.VMEM((tiles, LANES), jnp.bfloat16),
            pltpu.VMEM((tiles, LANES), jnp.bfloat16),
            dma((3,)),
            pltpu.VMEM((rows, local_features), jnp.int32),
            pltpu.VMEM((n, own, rows), jnp.bfloat16),
            pltpu.VMEM((n_feat, meta_rows, LANES), jnp.bfloat16),
            pltpu.VMEM((n, own, rows), jnp.bfloat16),
            pltpu.VMEM((n_feat, n, meta_rows, LANES), jnp.bfloat16),
            pltpu.VMEM((2 * LEAVES, rows), jnp.bfloat16),
            pltpu.VMEM((own, 4 * LEAVES, HALF), jnp.float32),
            pltpu.VMEM((1, LANES), jnp.float32),
            pltpu.VMEM((everyone, 1, LANES), jnp.float32),
            dma((pieces,)), dma((n,)), dma((n,)), dma((n,)), dma((n,)), dma((n_feat,)), dma((n_feat,)), dma((2,)),
            dma((everyone,)), dma((everyone,)),
        ],
        compiler_params=pltpu.CompilerParams(
            collective_id=0, has_side_effects=True, vmem_limit_bytes=60 * 1024 * 1024),
    )(bin_index, leaf_ids.reshape(tiles, LANES), gradients.reshape(tiles, LANES), hessians.reshape(tiles, LANES))
    return gain[None], best.reshape(LEAVES)


def solution(mesh):
    placed = (P("rows", "feat"), P("rows"), P("rows"), P("rows"))
    return jax.shard_map(
        body,
        mesh=mesh,
        in_specs=placed,
        out_specs=(P("feat", "rows", None, None), P()),
        check_vma=False,
    )
```

```python
import functools

import jax
import jax.numpy as jnp
from jax import lax
from jax.experimental import pallas as pl
from jax.experimental.pallas import tpu as pltpu
from jax.sharding import PartitionSpec as P

BINS = 256
LEAVES = 16
LANES = 128
HALF = BINS // 2
DEPTH = 256
MESH = pl.DeviceIdType.MESH

reg_lambda = 1.0


def kernel(n, n_feat, bins_hbm, leaf_hbm, grad_hbm, hess_hbm, gain_ref, best_ref,
           leaf_ref, grad_ref, hess_ref, small_sems, raw, bins_src, meta_src, columns, metas, weights, top, landing,
           raw_sems, bin_send, bin_recv, meta_send, meta_recv, swap_send, swap_recv, own_sems, top_send, top_recv):
    me, me_feat = lax.axis_index("rows"), lax.axis_index("feat")
    everyone = n * n_feat
    me_all = me * n_feat + me_feat
    own, rows = bins_src.shape[1], bins_src.shape[2]
    tiles = rows // LANES
    share = tiles // n_feat
    half = n // 2
    across = (1 - me // half) * half
    pieces = raw_sems.shape[0]
    piece_rows = rows // pieces

    def fetch(piece):
        span = pl.ds(piece * piece_rows, piece_rows)
        return pltpu.make_async_copy(bins_hbm.at[span], raw.at[span], raw_sems.at[piece])

    small = [pltpu.make_async_copy(source, target, small_sems.at[place]) for place, (source, target) in enumerate(
        ((leaf_hbm, leaf_ref), (grad_hbm, grad_ref), (hess_hbm, hess_ref)))]
    for copy in small:
        copy.start()
    for piece in range(pieces):
        fetch(piece).start()

    def partner(step):
        other, bit = 0, 1
        while bit < n:
            other += lax.rem(me // bit + step // bit, 2) * bit
            bit *= 2
        return other

    def device_after(step):
        return {"rows": partner(step // n_feat), "feat": lax.rem(me_feat + lax.rem(step, n_feat), n_feat)}

    barrier = pltpu.get_barrier_semaphore()

    def each(first, last, act):
        def run(step, carry):
            act(step)
            return carry
        lax.fori_loop(first, last, run, 0, unroll=everyone <= 64)

    def greet(device):
        pl.semaphore_signal(barrier, inc=1, device_id=device, device_id_type=MESH)

    each(1, n, lambda step: greet({"rows": partner(n - step)}))
    each(1, n_feat, lambda step: greet(device_after(step)))

    for copy in small:
        copy.wait()
    leaf, grad, hess = (ref[...].astype(jnp.float32) for ref in (leaf_ref, grad_ref, hess_ref))
    spare = jnp.zeros((meta_src.shape[1] - 3 * share, LANES), jnp.float32)
    for part in range(n_feat):
        span = slice(part * share, (part + 1) * share)
        meta_src[part] = jnp.concatenate([leaf[span], grad[span], hess[span], spare], axis=0).astype(jnp.bfloat16)
    for piece in range(pieces):
        fetch(piece).wait()
        for tile in range(piece * piece_rows // LANES, (piece + 1) * piece_rows // LANES):
            lanes = slice(tile * LANES, (tile + 1) * LANES)
            turned = raw[lanes].astype(jnp.float32).T.astype(jnp.bfloat16)
            bins_src[:, :, lanes] = turned.reshape(n, own, LANES)

    own_bins = pltpu.make_async_copy(bins_src.at[me], columns.at[me], own_sems.at[0])
    own_meta = pltpu.make_async_copy(meta_src, metas.at[:, me], own_sems.at[1])
    own_bins.start()
    own_meta.start()
    pl.semaphore_wait(barrier, n - 1 + n_feat - 1)

    def bin_copy(step, landed):
        other = partner(step)
        return pltpu.make_async_remote_copy(
            src_ref=bins_src.at[other], dst_ref=columns.at[other if landed else me], send_sem=bin_send.at[step],
            recv_sem=bin_recv.at[step], device_id={"rows": other}, device_id_type=MESH)

    def near_meta(step, landed):
        other = partner(step)
        return pltpu.make_async_remote_copy(
            src_ref=meta_src, dst_ref=metas.at[:, other if landed else me], send_sem=meta_send.at[step],
            recv_sem=meta_recv.at[step], device_id={"rows": other}, device_id_type=MESH)

    def far_meta(step, landed):
        other = partner(step)
        return pltpu.make_async_remote_copy(
            src_ref=meta_src.at[me_feat], dst_ref=metas.at[me_feat, other if landed else me], send_sem=meta_send.at[step],
            recv_sem=meta_recv.at[step], device_id={"rows": other}, device_id_type=MESH)

    def swap_meta(step, landed):
        held = lax.rem(me_feat + n_feat - step, n_feat) if landed else me_feat
        far = metas.at[held, pl.ds(across, half)]
        return pltpu.make_async_remote_copy(
            src_ref=far, dst_ref=far, send_sem=swap_send.at[step], recv_sem=swap_recv.at[step],
            device_id={"feat": lax.rem(me_feat + step, n_feat)}, device_id_type=MESH)

    each(half, n, lambda step: far_meta(step, False).start())
    each(1, half, lambda step: near_meta(step, False).start())
    each(1, n, lambda step: bin_copy(step, False).start())
    landing[0] = jnp.full((1, LANES), -jnp.inf, jnp.float32)
    own_bins.wait()
    own_meta.wait()

    pairs = -(-own // 2)

    def compute(*sums):
        for total in sums:
            pltpu.matmul_pop(total)
        lax.fori_loop(0, n, functools.partial(one_shard, sums), 0)
        largest = jnp.full((LEAVES, HALF), -jnp.inf, jnp.float32)
        for pair in range(pairs):
            largest = gains(pair, pltpu.matmul_pop(sums[pair]), largest)
        largest = jnp.broadcast_to(jnp.max(largest, axis=1, keepdims=True), (LEAVES, LANES))
        on_lane = (lax.broadcasted_iota(jnp.int32, (LEAVES, LANES), 0)
                   == lax.broadcasted_iota(jnp.int32, (LEAVES, LANES), 1))
        top[...] = jnp.max(jnp.where(on_lane, largest, -jnp.inf), axis=0, keepdims=True)

    def one_shard(sums, step, carry):
        origin = partner(step)

        @pl.when(step == min(2, half - 1))
        def swap():
            each(half, n, lambda far: far_meta(far, True).wait_recv())
            each(1, n_feat, lambda other: swap_meta(other, False).start())

        @pl.when(jnp.logical_and(step > 0, step < half))
        def near_arrived():
            near_meta(step, True).wait_recv()

        @pl.when(step == half)
        def swapped():
            each(1, n_feat, lambda other: swap_meta(other, True).wait_recv())

        @pl.when(step > 0)
        def arrived():
            bin_copy(step, True).wait_recv()

        table = metas[:, origin].astype(jnp.float32)
        leaf_of = lax.broadcasted_iota(jnp.int32, (LEAVES, LANES), 0).astype(jnp.float32)
        for tile in range(tiles):
            piece, row = tile // share, tile % share
            member = jnp.broadcast_to(table[piece, row:row + 1], (LEAVES, LANES)) == leaf_of
            for part in (0, 1):
                first = (1 + part) * share + row
                value = jnp.broadcast_to(table[piece, first:first + 1], (LEAVES, LANES))
                weights[part * LEAVES:(part + 1) * LEAVES, tile * LANES:(tile + 1) * LANES] = (
                    jnp.where(member, value, 0.0).astype(jnp.bfloat16))

        block = columns[origin]
        low = jnp.where(block >= HALF, block - HALF, block)
        level = lax.broadcasted_iota(jnp.int32, (HALF, DEPTH), 0).astype(jnp.bfloat16)
        zero = jnp.zeros((), jnp.bfloat16)
        hit, miss = (jnp.full((HALF, DEPTH), value, jnp.float8_e4m3fn) for value in (1, 0))

        def step_of(feature, lanes):
            reached = jnp.broadcast_to(low[feature:feature + 1, lanes], (HALF, DEPTH)) <= level
            return jnp.where(reached, hit, miss)

        def upper_of(feature, lanes, table_rows):
            upper = jnp.broadcast_to(block[feature:feature + 1, lanes], (2 * LEAVES, DEPTH)) >= HALF
            return jnp.where(upper, table_rows, zero)

        for first in range(0, pairs, 2):
            for chunk in range(rows // DEPTH):
                lanes = slice(chunk * DEPTH, (chunk + 1) * DEPTH)
                table_rows = weights[:, lanes]
                for pair in range(first, min(first + 2, pairs)):
                    features = (2 * pair, min(2 * pair + 1, own - 1))
                    steps = jnp.concatenate([step_of(feature, lanes) for feature in features], axis=0)
                    turned = (chunk + pair) % 3 != 0
                    pltpu.matmul_push_rhs(
                        steps.T if turned else steps,
                        staging_register=chunk % 2, mxu_index=pair % 2, transpose=not turned)
                    pltpu.matmul_acc_lhs(
                        sums[pair],
                        jnp.concatenate([table_rows] + [upper_of(feature, lanes, table_rows) for feature in features], axis=0),
                        load_staged_rhs=chunk % 2)
        return carry

    def gains(pair, part, largest):
        for place in range(2):
            feature = 2 * pair + place
            if feature == own:
                break
            lanes = slice(place * HALF, (place + 1) * HALF)
            both = part[:2 * LEAVES, lanes]
            upper = part[(1 + place) * 2 * LEAVES:(2 + place) * 2 * LEAVES, lanes]
            lower = both - upper
            grad_low, hess_low = lower[:LEAVES], lower[LEAVES:]
            grad_high = upper[:LEAVES] + grad_low[:, HALF - 1:]
            hess_high = upper[LEAVES:] + hess_low[:, HALF - 1:]
            total_grad, total_hess = grad_high[:, HALF - 1:], hess_high[:, HALF - 1:]
            whole = total_grad * total_grad / (total_hess + reg_lambda)
            for side, left_grad, left_hess in ((0, grad_low, hess_low), (1, grad_high, hess_high)):
                right_grad, right_hess = total_grad - left_grad, total_hess - left_hess
                gain = 0.5 * (left_grad * left_grad / (left_hess + reg_lambda)
                              + right_grad * right_grad / (right_hess + reg_lambda) - whole)
                gain_ref[feature, :, side * HALF:(side + 1) * HALF] = gain
                largest = jnp.maximum(largest, gain)
        return largest

    pl.run_scoped(compute, *[pltpu.ACC(pair % 2)((6 * LEAVES, 2 * HALF), jnp.float32) for pair in range(pairs)])

    def report(place):
        step = everyone - place
        return pltpu.make_async_remote_copy(
            src_ref=top, dst_ref=landing.at[step], send_sem=top_send.at[step],
            recv_sem=top_recv.at[step], device_id=device_after(step), device_id_type=MESH)

    each(1, everyone, lambda place: report(place).start())
    each(1, n, lambda step: bin_copy(step, False).wait_send())
    each(1, half, lambda step: near_meta(step, False).wait_send())
    each(half, n, lambda step: far_meta(step, False).wait_send())
    each(1, n_feat, lambda step: swap_meta(step, False).wait_send())
    each(1, everyone, lambda place: report(everyone - place).wait_recv())
    best = jnp.maximum(top[...], jnp.max(landing[...], axis=0))
    each(1, everyone, lambda step: report(step).wait_send())
    best_ref[...] = best[:, :LEAVES]


def body(bin_index, leaf_ids, gradients, hessians):
    n, n_feat = lax.axis_size("rows"), lax.axis_size("feat")
    rows, local_features = bin_index.shape
    own = local_features // n
    tiles = rows // LANES
    pieces = 4
    everyone = n * n_feat
    meta_rows = -(-3 * (tiles // n_feat) // 16) * 16
    vmem = pl.BlockSpec(memory_space=pltpu.VMEM)
    dma = pltpu.SemaphoreType.DMA
    gain, best = pl.pallas_call(
        functools.partial(kernel, n, n_feat),
        out_shape=(pltpu.VMEM((own, LEAVES, BINS), jnp.float32),
                   pltpu.VMEM((1, LEAVES), jnp.float32)),
        in_specs=[pl.BlockSpec(memory_space=pl.ANY)] * 4,
        out_specs=(vmem, vmem),
        scratch_shapes=[
            pltpu.VMEM((tiles, LANES), jnp.int32),
            pltpu.VMEM((tiles, LANES), jnp.bfloat16),
            pltpu.VMEM((tiles, LANES), jnp.bfloat16),
            dma((3,)),
            pltpu.VMEM((rows, local_features), jnp.int32),
            pltpu.VMEM((n, own, rows), jnp.bfloat16),
            pltpu.VMEM((n_feat, meta_rows, LANES), jnp.bfloat16),
            pltpu.VMEM((n, own, rows), jnp.bfloat16),
            pltpu.VMEM((n_feat, n, meta_rows, LANES), jnp.bfloat16),
            pltpu.VMEM((2 * LEAVES, rows), jnp.bfloat16),
            pltpu.VMEM((1, LANES), jnp.float32),
            pltpu.VMEM((everyone, 1, LANES), jnp.float32),
            dma((pieces,)), dma((n,)), dma((n,)), dma((n,)), dma((n,)), dma((n_feat,)), dma((n_feat,)), dma((2,)),
            dma((everyone,)), dma((everyone,)),
        ],
        compiler_params=pltpu.CompilerParams(
            collective_id=0, has_side_effects=True, vmem_limit_bytes=60 * 1024 * 1024),
    )(bin_index, leaf_ids.reshape(tiles, LANES), gradients.reshape(tiles, LANES), hessians.reshape(tiles, LANES))
    return gain[None], best.reshape(LEAVES)


def solution(mesh):
    placed = (P("rows", "feat"), P("rows"), P("rows"), P("rows"))
    return jax.shard_map(
        body,
        mesh=mesh,
        in_specs=placed,
        out_specs=(P("feat", "rows", None, None), P()),
        check_vma=False,
    )
```

```python
import functools

import jax
import jax.numpy as jnp
from jax import lax
from jax.experimental import pallas as pl
from jax.experimental.pallas import tpu as pltpu
from jax.sharding import PartitionSpec as P

BINS = 256
LEAVES = 16
LANES = 128
HALF = BINS // 2
DEPTH = 256
MESH = pl.DeviceIdType.MESH

reg_lambda = 1.0


def kernel(n, n_feat, bins_hbm, leaf_hbm, grad_hbm, hess_hbm, gain_ref, best_ref,
           leaf_ref, grad_ref, hess_ref, small_sems, raw, bins_src, meta_src, columns, metas, weights, top, landing,
           raw_sems, bin_send, bin_recv, near_send, near_recv, far_send, far_recv, swap_send, swap_recv, own_sems,
           top_send, top_recv):
    me, me_feat = lax.axis_index("rows"), lax.axis_index("feat")
    everyone = n * n_feat
    me_all = me * n_feat + me_feat
    own, rows = bins_src.shape[1], bins_src.shape[2]
    tiles = rows // LANES
    share = tiles // n_feat
    half, quarter = n // 2, n // 4
    across = (1 - me // half) * half
    pieces = raw_sems.shape[0]
    piece_rows = rows // pieces

    def fetch(piece):
        span = pl.ds(piece * piece_rows, piece_rows)
        return pltpu.make_async_copy(bins_hbm.at[span], raw.at[span], raw_sems.at[piece])

    small = [pltpu.make_async_copy(source, target, small_sems.at[place]) for place, (source, target) in enumerate(
        ((leaf_hbm, leaf_ref), (grad_hbm, grad_ref), (hess_hbm, hess_ref)))]
    for copy in small:
        copy.start()
    for piece in range(pieces):
        fetch(piece).start()

    def partner(step):
        other, bit = 0, 1
        while bit < n:
            other += lax.rem(me // bit + step // bit, 2) * bit
            bit *= 2
        return other

    def device_after(step):
        return {"rows": partner(step // n_feat), "feat": lax.rem(me_feat + lax.rem(step, n_feat), n_feat)}

    barrier = pltpu.get_barrier_semaphore()

    def each(first, last, act):
        def run(step, carry):
            act(step)
            return carry
        lax.fori_loop(first, last, run, 0, unroll=everyone <= 64)

    def greet(device):
        pl.semaphore_signal(barrier, inc=1, device_id=device, device_id_type=MESH)

    each(1, n, lambda step: greet({"rows": partner(n - step)}))
    each(1, n_feat, lambda step: greet(device_after(step)))

    for copy in small:
        copy.wait()
    leaf, grad, hess = (ref[...].astype(jnp.float32) for ref in (leaf_ref, grad_ref, hess_ref))
    spare = jnp.zeros((meta_src.shape[1] - 3 * share, LANES), jnp.float32)
    for part in range(n_feat):
        span = slice(part * share, (part + 1) * share)
        meta_src[part] = jnp.concatenate([leaf[span], grad[span], hess[span], spare], axis=0).astype(jnp.bfloat16)
    for piece in range(pieces):
        fetch(piece).wait()
        for tile in range(piece * piece_rows // LANES, (piece + 1) * piece_rows // LANES):
            lanes = slice(tile * LANES, (tile + 1) * LANES)
            turned = raw[lanes].astype(jnp.float32).astype(jnp.bfloat16).T
            bins_src[:, :, lanes] = turned.reshape(n, own, LANES)

    own_bins = pltpu.make_async_copy(bins_src.at[me], columns.at[me], own_sems.at[0])
    own_meta = pltpu.make_async_copy(meta_src, metas.at[:, me], own_sems.at[1])
    own_bins.start()
    own_meta.start()
    pl.semaphore_wait(barrier, n - 1 + n_feat - 1)

    def bin_copy(step, landed):
        other = partner(step)
        return pltpu.make_async_remote_copy(
            src_ref=bins_src.at[other], dst_ref=columns.at[other if landed else me], send_sem=bin_send,
            recv_sem=bin_recv.at[step], device_id={"rows": other}, device_id_type=MESH)

    def late_copy(step, part, landed):
        other = partner(step)
        some = pl.ds(part * (rows // 2), rows // 2)
        return pltpu.make_async_remote_copy(
            src_ref=bins_src.at[other, :, some], dst_ref=columns.at[other if landed else me, :, some],
            send_sem=bin_send, recv_sem=bin_recv.at[step + 2 * part],
            device_id={"rows": other}, device_id_type=MESH)

    def use_step(place):
        later = place - 2
        turns = jnp.where(later % 2 == 0, 2 + later // 2, half + later // 2)
        near_left = 2 + later - quarter
        step = jnp.where(later < 2 * quarter, turns, jnp.where(place < half + quarter, near_left, place))
        return jnp.where(later < 0, place, step)

    def send_step(place):
        turns = 1 + place // 2 + (place % 2) * (half - 1)
        return jnp.where(place < half, turns, jnp.where(place < half + quarter - 1, 1 + place - quarter, place + 1))

    def near_meta(step, landed):
        other = partner(step)
        return pltpu.make_async_remote_copy(
            src_ref=meta_src, dst_ref=metas.at[:, other if landed else me], send_sem=near_send,
            recv_sem=near_recv.at[step], device_id={"rows": other}, device_id_type=MESH)

    def far_meta(step, landed):
        other = partner(step)
        return pltpu.make_async_remote_copy(
            src_ref=meta_src.at[me_feat], dst_ref=metas.at[me_feat, other if landed else me], send_sem=far_send,
            recv_sem=far_recv, device_id={"rows": other}, device_id_type=MESH)

    far_rows = metas.at[0, pl.ds(0, half)]
    near_rows = metas.at[:, pl.ds(0, half - 1)]
    swapped_rows = metas.at[pl.ds(0, n_feat - 1), pl.ds(0, half)]
    sent_blocks = columns.at[pl.ds(0, n - 1)]
    reports = landing.at[pl.ds(1, everyone - 1)]

    def swap_meta(step, landed):
        held = lax.rem(me_feat + n_feat - step, n_feat) if landed else me_feat
        far = metas.at[held, pl.ds(across, half)]
        return pltpu.make_async_remote_copy(
            src_ref=far, dst_ref=far, send_sem=swap_send, recv_sem=swap_recv,
            device_id={"feat": lax.rem(me_feat + step, n_feat)}, device_id_type=MESH)

    each(half, n, lambda step: far_meta(step, False).start())
    each(1, half, lambda step: near_meta(step, False).start())
    each(0, n - 3, lambda place: bin_copy(send_step(place), False).start())
    late = [(step, part) for part in range(2) for step in (n - 2, n - 1)]
    for step, part in late:
        late_copy(step, part, False).start()
    landing[0] = jnp.full((1, LANES), -jnp.inf, jnp.float32)
    own_bins.wait()
    own_meta.wait()

    pairs = -(-own // 2)

    def compute(*sums):
        for total in sums:
            pltpu.matmul_pop(total)
        lax.fori_loop(0, n - 2, functools.partial(one_shard, sums), 0)
        for step, part in late:
            late_copy(step, part, True).wait_recv()
            add_rows(sums, partner(step), part * (tiles // 2), (part + 1) * (tiles // 2))
        for refs, sem in ((sent_blocks, bin_send), (near_rows, near_send), (far_rows, far_send), (swapped_rows, swap_send)):
            pltpu.make_async_copy(refs, refs, sem).wait()
        largest = jnp.full((LEAVES, HALF), -jnp.inf, jnp.float32)
        for pair in range(pairs):
            largest = gains(pair, pltpu.matmul_pop(sums[pair]), largest)
        largest = jnp.broadcast_to(jnp.max(largest, axis=1, keepdims=True), (LEAVES, LANES))
        on_lane = (lax.broadcasted_iota(jnp.int32, (LEAVES, LANES), 0)
                   == lax.broadcasted_iota(jnp.int32, (LEAVES, LANES), 1))
        top[...] = jnp.max(jnp.where(on_lane, largest, -jnp.inf), axis=0, keepdims=True)

    def one_shard(sums, place, carry):
        step = use_step(place)
        origin = partner(step)

        @pl.when(place == 2)
        def swap():
            pltpu.make_async_copy(far_rows, far_rows, far_recv).wait()
            each(1, n_feat, lambda other: swap_meta(other, False).start())

        @pl.when(jnp.logical_and(step > 0, step < half))
        def near_arrived():
            near_meta(step, True).wait_recv()

        @pl.when(place == 3)
        def swapped():
            pltpu.make_async_copy(swapped_rows, swapped_rows, swap_recv).wait()

        @pl.when(step > 0)
        def arrived():
            bin_copy(step, True).wait_recv()

        add_rows(sums, origin, 0, tiles)
        return carry

    def add_rows(sums, origin, first_tile, last_tile):
        table = metas[:, origin].astype(jnp.float32)
        leaf_of = lax.broadcasted_iota(jnp.int32, (LEAVES, LANES), 0).astype(jnp.float32)
        for tile in range(first_tile, last_tile):
            piece, row = tile // share, tile % share
            member = jnp.broadcast_to(table[piece, row:row + 1], (LEAVES, LANES)) == leaf_of
            for part in (0, 1):
                first = (1 + part) * share + row
                value = jnp.broadcast_to(table[piece, first:first + 1], (LEAVES, LANES))
                weights[part * LEAVES:(part + 1) * LEAVES, tile * LANES:(tile + 1) * LANES] = (
                    jnp.where(member, value, 0.0).astype(jnp.bfloat16))

        begin = first_tile * LANES
        block = columns[origin, :, begin:last_tile * LANES]
        low = jnp.where(block >= HALF, block - HALF, block)
        level = lax.broadcasted_iota(jnp.int32, (HALF, DEPTH), 0).astype(jnp.bfloat16)
        zero = jnp.zeros((), jnp.bfloat16)
        hit, miss = (jnp.full((HALF, DEPTH), value, jnp.float8_e4m3fn) for value in (1, 0))

        def step_of(feature, lanes):
            reached = jnp.broadcast_to(low[feature:feature + 1, lanes], (HALF, DEPTH)) <= level
            return jnp.where(reached, hit, miss)

        def upper_of(feature, lanes, table_rows):
            upper = jnp.broadcast_to(block[feature:feature + 1, lanes], (2 * LEAVES, DEPTH)) >= HALF
            return jnp.where(upper, table_rows, zero)

        for first in range(0, pairs, 2):
            for chunk in range(block.shape[1] // DEPTH):
                lanes = slice(chunk * DEPTH, (chunk + 1) * DEPTH)
                table_rows = weights[:, begin + chunk * DEPTH:begin + (chunk + 1) * DEPTH]
                for pair in range(first, min(first + 2, pairs)):
                    features = (2 * pair, min(2 * pair + 1, own - 1))
                    steps = jnp.concatenate([step_of(feature, lanes) for feature in features], axis=0)
                    turned = (chunk + pair) % 3 != 0
                    pltpu.matmul_push_rhs(
                        steps.T if turned else steps,
                        staging_register=chunk % 2, mxu_index=pair % 2, transpose=not turned)
                    pltpu.matmul_acc_lhs(
                        sums[pair],
                        jnp.concatenate([table_rows] + [upper_of(feature, lanes, table_rows) for feature in features], axis=0),
                        load_staged_rhs=chunk % 2)

    def gains(pair, part, largest):
        for place in range(2):
            feature = 2 * pair + place
            if feature == own:
                break
            lanes = slice(place * HALF, (place + 1) * HALF)
            both = part[:2 * LEAVES, lanes]
            upper = part[(1 + place) * 2 * LEAVES:(2 + place) * 2 * LEAVES, lanes]
            total = both[:, HALF - 1:]
            lower, beyond = both - upper, upper[:, HALF - 1:] - upper
            total_grad, total_hess = total[:LEAVES], total[LEAVES:]
            whole = total_grad * total_grad / (total_hess + reg_lambda)
            for side, left, right in ((0, lower, total - lower), (1, total - beyond, beyond)):
                left_grad, left_hess = left[:LEAVES], left[LEAVES:]
                right_grad, right_hess = right[:LEAVES], right[LEAVES:]
                gain = 0.5 * (left_grad * left_grad / (left_hess + reg_lambda)
                              + right_grad * right_grad / (right_hess + reg_lambda) - whole)
                gain_ref[feature, :, side * HALF:(side + 1) * HALF] = gain
                largest = jnp.maximum(largest, gain)
        return largest

    pl.run_scoped(compute, *[pltpu.ACC(pair % 2)((6 * LEAVES, 2 * HALF), jnp.float32) for pair in range(pairs)])

    def report(place):
        step = everyone - place
        return pltpu.make_async_remote_copy(
            src_ref=top, dst_ref=landing.at[step], send_sem=top_send,
            recv_sem=top_recv, device_id=device_after(step), device_id_type=MESH)

    each(1, everyone, lambda place: report(place).start())
    pltpu.make_async_copy(reports, reports, top_recv).wait()
    best = jnp.maximum(top[...], jnp.max(landing[...], axis=0))
    pltpu.make_async_copy(reports, reports, top_send).wait()
    best_ref[...] = best[:, :LEAVES]


def body(bin_index, leaf_ids, gradients, hessians):
    n, n_feat = lax.axis_size("rows"), lax.axis_size("feat")
    rows, local_features = bin_index.shape
    own = local_features // n
    tiles = rows // LANES
    pieces = 1
    everyone = n * n_feat
    half = n // 2
    meta_rows = -(-3 * (tiles // n_feat) // 16) * 16
    vmem = pl.BlockSpec(memory_space=pltpu.VMEM)
    dma = pltpu.SemaphoreType.DMA
    gain, best = pl.pallas_call(
        functools.partial(kernel, n, n_feat),
        out_shape=(pltpu.VMEM((own, LEAVES, BINS), jnp.float32),
                   pltpu.VMEM((1, LEAVES), jnp.float32)),
        in_specs=[pl.BlockSpec(memory_space=pl.ANY)] * 4,
        out_specs=(vmem, vmem),
        scratch_shapes=[
            pltpu.VMEM((tiles, LANES), jnp.int32),
            pltpu.VMEM((tiles, LANES), jnp.bfloat16),
            pltpu.VMEM((tiles, LANES), jnp.bfloat16),
            dma((3,)),
            pltpu.VMEM((rows, local_features), jnp.int32),
            pltpu.VMEM((n, own, rows), jnp.bfloat16),
            pltpu.VMEM((n_feat, meta_rows, LANES), jnp.bfloat16),
            pltpu.VMEM((n, own, rows), jnp.bfloat16),
            pltpu.VMEM((n_feat, n, meta_rows, LANES), jnp.bfloat16),
            pltpu.VMEM((2 * LEAVES, rows), jnp.bfloat16),
            pltpu.VMEM((1, LANES), jnp.float32),
            pltpu.VMEM((everyone, 1, LANES), jnp.float32),
            dma((pieces,)), dma, dma((n + 2,)), dma, dma((half,)), dma, dma, dma, dma, dma((2,)), dma, dma,
        ],
        compiler_params=pltpu.CompilerParams(
            collective_id=0, has_side_effects=True, vmem_limit_bytes=60 * 1024 * 1024),
    )(bin_index, leaf_ids.reshape(tiles, LANES), gradients.reshape(tiles, LANES), hessians.reshape(tiles, LANES))
    return gain[None], best.reshape(LEAVES)


def solution(mesh):
    placed = (P("rows", "feat"), P("rows"), P("rows"), P("rows"))
    return jax.shard_map(
        body,
        mesh=mesh,
        in_specs=placed,
        out_specs=(P("feat", "rows", None, None), P()),
        check_vma=False,
    )
```

```python
import functools

import jax
import jax.numpy as jnp
from jax import lax
from jax.experimental import pallas as pl
from jax.experimental.pallas import tpu as pltpu
from jax.sharding import PartitionSpec as P

BINS = 256
LEAVES = 16
LANES = 128
HALF = BINS // 2
DEPTH = 256
MESH = pl.DeviceIdType.MESH

reg_lambda = 1.0


def kernel(n, n_feat, bins_hbm, leaf_hbm, grad_hbm, hess_hbm, gain_ref, best_ref,
           leaf_ref, grad_ref, hess_ref, small_sems, raw, bins_src, meta_src, columns, metas, weights, top, landing,
           raw_sems, bin_send, bin_recv, near_send, near_recv, far_send, far_recv, swap_send, swap_recv, own_sems,
           top_send, top_recv, side_in, tally):
    me, me_feat = lax.axis_index("rows"), lax.axis_index("feat")
    everyone = n * n_feat
    me_all = me * n_feat + me_feat
    own, rows = bins_src.shape[1], bins_src.shape[2]
    tiles = rows // LANES
    share = tiles // n_feat
    half, quarter = n // 2, n // 4
    side, across = me % 2, (1 - me // half) * quarter
    pieces = raw_sems.shape[0]
    piece_rows = rows // pieces

    def fetch(piece, first=0, count=piece_rows):
        span = pl.ds(piece * piece_rows + first, count)
        return pltpu.make_async_copy(bins_hbm.at[span], raw.at[span], raw_sems.at[piece])

    small = [pltpu.make_async_copy(source, target, small_sems.at[place]) for place, (source, target) in enumerate(
        ((leaf_hbm, leaf_ref), (grad_hbm, grad_ref), (hess_hbm, hess_ref)))]
    for copy in small:
        copy.start()
    for piece in range(pieces):
        for first in range(0, piece_rows, 2 * LANES):
            fetch(piece, first, 2 * LANES).start()

    def partner(step):
        other, bit = 0, 1
        while bit < n:
            other += lax.rem(me // bit + step // bit, 2) * bit
            bit *= 2
        return other

    def device_after(step):
        return {"rows": partner(step // n_feat), "feat": lax.rem(me_feat + lax.rem(step, n_feat), n_feat)}

    barrier = pltpu.get_barrier_semaphore()

    def each(first, last, act):
        def run(step, carry):
            act(step)
            return carry
        lax.fori_loop(first, last, run, 0, unroll=everyone <= 64)

    def greet(device):
        pl.semaphore_signal(barrier, inc=1, device_id=device, device_id_type=MESH)

    each(1, half, lambda turn: greet({"rows": partner(n - 2 * turn)}))
    greet({"rows": partner(1)})
    each(1, n_feat, lambda step: greet(device_after(step)))

    for copy in small:
        copy.wait()
    leaf, grad, hess = (ref[...].astype(jnp.float32) for ref in (leaf_ref, grad_ref, hess_ref))
    spare = jnp.zeros((meta_src.shape[1] - 3 * share, LANES), jnp.float32)
    for part in range(n_feat):
        span = slice(part * share, (part + 1) * share)
        meta_src[part] = jnp.concatenate([leaf[span], grad[span], hess[span], spare], axis=0).astype(jnp.bfloat16)
    for piece in range(pieces):
        fetch(piece).wait()
        for tile in range(piece * piece_rows // LANES, (piece + 1) * piece_rows // LANES):
            lanes = slice(tile * LANES, (tile + 1) * LANES)
            turned = raw[lanes].astype(jnp.float32).astype(jnp.bfloat16).T
            bins_src[:, :, lanes] = turned.reshape(n, own, LANES)

    own_bins = pltpu.make_async_copy(bins_src.at[me], columns.at[me], own_sems.at[0])
    own_meta = pltpu.make_async_copy(meta_src, metas.at[:, me % 2, me // 2], own_sems.at[1])
    own_bins.start()
    own_meta.start()
    pl.semaphore_wait(barrier, half + n_feat - 1)

    def bin_copy(step, landed):
        other = partner(step)
        return pltpu.make_async_remote_copy(
            src_ref=bins_src.at[other], dst_ref=columns.at[other if landed else me], send_sem=bin_send,
            recv_sem=bin_recv.at[step], device_id={"rows": other}, device_id_type=MESH)

    def late_copy(step, part, landed):
        other = partner(step)
        some = pl.ds(part * (rows // 2), rows // 2)
        return pltpu.make_async_remote_copy(
            src_ref=bins_src.at[other, :, some], dst_ref=columns.at[other if landed else me, :, some],
            send_sem=bin_send, recv_sem=bin_recv.at[step + 2 * part],
            device_id={"rows": other}, device_id_type=MESH)

    def use_step(place):
        later = place - 2
        turns = jnp.where(later % 2 == 0, 2 + later // 2, half + later // 2)
        near_left = 2 + later - quarter
        step = jnp.where(later < 2 * quarter, turns, jnp.where(place < half + quarter, near_left, place))
        return jnp.where(later < 0, place, step)

    def send_step(place):
        turns = 1 + place // 2 + (place % 2) * (half - 1)
        return jnp.where(place < half, turns, jnp.where(place < half + quarter - 1, 1 + place - quarter, place + 1))

    def near_meta(step, landed):
        other = partner(step)
        row = other if landed else me
        return pltpu.make_async_remote_copy(
            src_ref=meta_src, dst_ref=metas.at[:, row % 2, row // 2], send_sem=near_send,
            recv_sem=near_recv.at[step], device_id={"rows": other}, device_id_type=MESH)

    def far_meta(step):
        return pltpu.make_async_remote_copy(
            src_ref=meta_src.at[me_feat], dst_ref=metas.at[me_feat, side, me // 2], send_sem=far_send,
            recv_sem=far_recv, device_id={"rows": partner(step)}, device_id_type=MESH)

    far_rows = metas.at[0, 0, pl.ds(0, quarter)]
    near_rows = metas.at[:, 0, pl.ds(0, half - 1)]
    sent_blocks = columns.at[pl.ds(0, n - 1)]
    reports = landing.at[pl.ds(1, everyone - 1)]

    def swap_meta(step):
        far = metas.at[me_feat, side, pl.ds(across, quarter)]
        return pltpu.make_async_remote_copy(
            src_ref=far, dst_ref=far, send_sem=swap_send, recv_sem=swap_recv,
            device_id={"rows": partner(1) if step >= n_feat else me, "feat": lax.rem(me_feat + step % n_feat, n_feat)},
            device_id_type=MESH)

    def await_swaps(sem):
        pltpu.make_async_copy(tally, tally, sem).wait()

    pl.semaphore_signal(side_in, inc=1, device_id={"rows": partner(1)}, device_id_type=MESH)
    each(quarter, half, lambda turn: far_meta(2 * turn).start())
    near_meta(1, False).start()
    each(1, quarter, lambda turn: near_meta(2 * turn, False).start())
    late = [(step, part) for part in range(2) for step in (n - 2, n - 1)]
    each(0, 2, lambda place: bin_copy(send_step(place), False).start())

    def send_rest():
        pl.semaphore_wait(side_in, 1)
        each(1, quarter, lambda turn: near_meta(2 * turn + 1, False).start())
        each(2, n - 3, lambda place: bin_copy(send_step(place), False).start())
        for step, part in late:
            late_copy(step, part, False).start()

    landing[0] = jnp.full((1, LANES), -jnp.inf, jnp.float32)
    own_bins.wait()
    own_meta.wait()

    pairs = -(-own // 2)

    def compute(*sums):
        for total in sums:
            pltpu.matmul_pop(total)
        lax.fori_loop(0, n - 2, functools.partial(one_shard, sums), 0)
        for step, part in sorted(late):
            late_copy(step, part, True).wait_recv()
            add_rows(sums, partner(step), part * (tiles // 2), (part + 1) * (tiles // 2))
        for refs, sem in ((sent_blocks, bin_send), (near_rows, near_send), (far_rows, far_send)):
            pltpu.make_async_copy(refs, refs, sem).wait()
        await_swaps(swap_send)
        largest = jnp.full((LEAVES, HALF), -jnp.inf, jnp.float32)
        for pair in range(pairs):
            largest = gains(pair, pltpu.matmul_pop(sums[pair]), largest)
        largest = jnp.broadcast_to(jnp.max(largest, axis=1, keepdims=True), (LEAVES, LANES))
        on_lane = (lax.broadcasted_iota(jnp.int32, (LEAVES, LANES), 0)
                   == lax.broadcasted_iota(jnp.int32, (LEAVES, LANES), 1))
        top[...] = jnp.max(jnp.where(on_lane, largest, -jnp.inf), axis=0, keepdims=True)

    def one_shard(sums, place, carry):
        step = use_step(place)
        origin = partner(step)

        pl.when(place == 1)(send_rest)

        @pl.when(place == 2)
        def swap():
            pltpu.make_async_copy(far_rows, far_rows, far_recv).wait()
            for other in range(1, 2 * n_feat):
                swap_meta(other).start()

        @pl.when(jnp.logical_and(step > 0, step < half))
        def near_arrived():
            near_meta(step, True).wait_recv()

        @pl.when(place == 3)
        def swapped():
            await_swaps(swap_recv)

        @pl.when(step > 0)
        def arrived():
            bin_copy(step, True).wait_recv()

        add_rows(sums, origin, 0, tiles)
        return carry

    def add_rows(sums, origin, first_tile, last_tile):
        table = metas[:, origin % 2, origin // 2].astype(jnp.float32)
        leaf_of = lax.broadcasted_iota(jnp.int32, (LEAVES, LANES), 0).astype(jnp.float32)
        for tile in range(first_tile, last_tile):
            piece, row = tile // share, tile % share
            member = jnp.broadcast_to(table[piece, row:row + 1], (LEAVES, LANES)) == leaf_of
            for part in (0, 1):
                first = (1 + part) * share + row
                value = jnp.broadcast_to(table[piece, first:first + 1], (LEAVES, LANES))
                weights[part * LEAVES:(part + 1) * LEAVES, tile * LANES:(tile + 1) * LANES] = (
                    jnp.where(member, value, 0.0).astype(jnp.bfloat16))

        begin = first_tile * LANES
        block = columns[origin, :, begin:last_tile * LANES]
        low = jnp.where(block >= HALF, block - HALF, block)
        level = lax.broadcasted_iota(jnp.int32, (HALF, DEPTH), 0).astype(jnp.bfloat16)
        zero = jnp.zeros((), jnp.bfloat16)
        hit, miss = (jnp.full((HALF, DEPTH), value, jnp.float8_e4m3fn) for value in (1, 0))

        def step_of(feature, lanes):
            reached = jnp.broadcast_to(low[feature:feature + 1, lanes], (HALF, DEPTH)) <= level
            return jnp.where(reached, hit, miss)

        def upper_of(feature, lanes, table_rows):
            upper = jnp.broadcast_to(block[feature:feature + 1, lanes], (2 * LEAVES, DEPTH)) >= HALF
            return jnp.where(upper, table_rows, zero)

        for first in range(0, pairs, 2):
            for chunk in range(block.shape[1] // DEPTH):
                lanes = slice(chunk * DEPTH, (chunk + 1) * DEPTH)
                table_rows = weights[:, begin + chunk * DEPTH:begin + (chunk + 1) * DEPTH]
                for pair in range(first, min(first + 2, pairs)):
                    features = (2 * pair, min(2 * pair + 1, own - 1))
                    steps = jnp.concatenate([step_of(feature, lanes) for feature in features], axis=0)
                    turned = (chunk + pair) % 3 != 0
                    pltpu.matmul_push_rhs(
                        steps.T if turned else steps,
                        staging_register=chunk % 2, mxu_index=pair % 2, transpose=not turned)
                    pltpu.matmul_acc_lhs(
                        sums[pair],
                        jnp.concatenate([table_rows] + [upper_of(feature, lanes, table_rows) for feature in features], axis=0),
                        load_staged_rhs=chunk % 2)

    def gains(pair, part, largest):
        for place in range(2):
            feature = 2 * pair + place
            if feature == own:
                break
            lanes = slice(place * HALF, (place + 1) * HALF)
            both = part[:2 * LEAVES, lanes]
            upper = part[(1 + place) * 2 * LEAVES:(2 + place) * 2 * LEAVES, lanes]
            total = both[:, HALF - 1:]
            lower, beyond = both - upper, upper[:, HALF - 1:] - upper
            total_grad, total_hess = total[:LEAVES], total[LEAVES:]
            whole = total_grad * total_grad / (total_hess + reg_lambda)
            for side, left, right in ((0, lower, total - lower), (1, total - beyond, beyond)):
                left_grad, left_hess = left[:LEAVES], left[LEAVES:]
                right_grad, right_hess = right[:LEAVES], right[LEAVES:]
                gain = 0.5 * (left_grad * left_grad / (left_hess + reg_lambda)
                              + right_grad * right_grad / (right_hess + reg_lambda) - whole)
                gain_ref[feature, :, side * HALF:(side + 1) * HALF] = gain
                largest = jnp.maximum(largest, gain)
        return largest

    pl.run_scoped(compute, *[pltpu.ACC(pair % 2)((6 * LEAVES, 2 * HALF), jnp.float32) for pair in range(pairs)])

    def report(place):
        step = everyone - place
        return pltpu.make_async_remote_copy(
            src_ref=top, dst_ref=landing.at[step], send_sem=top_send,
            recv_sem=top_recv, device_id=device_after(step), device_id_type=MESH)

    each(1, everyone, lambda place: report(place).start())
    pltpu.make_async_copy(reports, reports, top_recv).wait()
    best = jnp.maximum(top[...], jnp.max(landing[...], axis=0))
    pltpu.make_async_copy(reports, reports, top_send).wait()
    best_ref[...] = best[:, :LEAVES]


def body(bin_index, leaf_ids, gradients, hessians):
    n, n_feat = lax.axis_size("rows"), lax.axis_size("feat")
    rows, local_features = bin_index.shape
    own = local_features // n
    tiles = rows // LANES
    pieces = 2
    everyone = n * n_feat
    half = n // 2
    meta_rows = -(-3 * (tiles // n_feat) // 16) * 16
    vmem = pl.BlockSpec(memory_space=pltpu.VMEM)
    dma = pltpu.SemaphoreType.DMA
    gain, best = pl.pallas_call(
        functools.partial(kernel, n, n_feat),
        out_shape=(pltpu.VMEM((own, LEAVES, BINS), jnp.float32),
                   pltpu.VMEM((1, LEAVES), jnp.float32)),
        in_specs=[pl.BlockSpec(memory_space=pl.ANY)] * 4,
        out_specs=(vmem, vmem),
        scratch_shapes=[
            pltpu.VMEM((tiles, LANES), jnp.int32),
            pltpu.VMEM((tiles, LANES), jnp.bfloat16),
            pltpu.VMEM((tiles, LANES), jnp.bfloat16),
            dma((3,)),
            pltpu.VMEM((rows, local_features), jnp.int32),
            pltpu.VMEM((n, own, rows), jnp.bfloat16),
            pltpu.VMEM((n_feat, meta_rows, LANES), jnp.bfloat16),
            pltpu.VMEM((n, own, rows), jnp.bfloat16),
            pltpu.VMEM((n_feat, 2, half, meta_rows, LANES), jnp.bfloat16),
            pltpu.VMEM((2 * LEAVES, rows), jnp.bfloat16),
            pltpu.VMEM((1, LANES), jnp.float32),
            pltpu.VMEM((everyone, 1, LANES), jnp.float32),
            dma((pieces,)), dma, dma((n + 2,)), dma, dma((half,)), dma, dma, dma, dma, dma((2,)), dma, dma, pltpu.SemaphoreType.REGULAR,
            pltpu.VMEM((2 * n_feat - 1, n // 4, meta_rows, LANES), jnp.bfloat16),
        ],
        compiler_params=pltpu.CompilerParams(
            collective_id=0, has_side_effects=True, vmem_limit_bytes=60 * 1024 * 1024),
    )(bin_index, leaf_ids.reshape(tiles, LANES), gradients.reshape(tiles, LANES), hessians.reshape(tiles, LANES))
    return gain[None], best.reshape(LEAVES)


def solution(mesh):
    placed = (P("rows", "feat"), P("rows"), P("rows"), P("rows"))
    return jax.shard_map(
        body,
        mesh=mesh,
        in_specs=placed,
        out_specs=(P("feat", "rows", None, None), P()),
        check_vma=False,
    )
```

```python
import functools

import jax
import jax.numpy as jnp
from jax import lax
from jax.experimental import pallas as pl
from jax.experimental.pallas import tpu as pltpu
from jax.sharding import PartitionSpec as P

BINS = 256
LEAVES = 16
LANES = 128
HALF = BINS // 2
DEPTH = 256
MESH = pl.DeviceIdType.MESH

reg_lambda = 1.0


def kernel(n, n_feat, bins_hbm, leaf_hbm, grad_hbm, hess_hbm, gain_ref, best_ref,
           leaf_ref, grad_ref, hess_ref, small_sems, raw, bins_src, meta_src, columns, metas, weights, top, landing,
           raw_sems, bin_send, bin_recv, near_send, near_recv, far_send, far_recv, swap_send, swap_recv, own_sems,
           top_send, top_recv, side_in, tally):
    me, me_feat = lax.axis_index("rows"), lax.axis_index("feat")
    everyone = n * n_feat
    me_all = me * n_feat + me_feat
    own, rows = bins_src.shape[1], bins_src.shape[2]
    tiles = rows // LANES
    share = tiles // n_feat
    half, quarter = n // 2, n // 4
    side, across = me % 2, (1 - me // half) * quarter
    pieces = raw_sems.shape[0]
    piece_rows = rows // pieces

    def fetch(piece, first=0, count=piece_rows):
        span = pl.ds(piece * piece_rows + first, count)
        return pltpu.make_async_copy(bins_hbm.at[span], raw.at[span], raw_sems.at[piece])

    small = [pltpu.make_async_copy(source, target, small_sems.at[place]) for place, (source, target) in enumerate(
        ((leaf_hbm, leaf_ref), (grad_hbm, grad_ref), (hess_hbm, hess_ref)))]
    for copy in small:
        copy.start()
    for piece in range(pieces):
        for first in range(0, piece_rows, 2 * LANES):
            fetch(piece, first, 2 * LANES).start()

    def partner(step):
        other, bit = 0, 1
        while bit < n:
            other += lax.rem(me // bit + step // bit, 2) * bit
            bit *= 2
        return other

    def device_after(step):
        return {"rows": partner(step // n_feat), "feat": lax.rem(me_feat + lax.rem(step, n_feat), n_feat)}

    barrier = pltpu.get_barrier_semaphore()

    def each(first, last, act):
        def run(step, carry):
            act(step)
            return carry
        lax.fori_loop(first, last, run, 0, unroll=everyone <= 64)

    def greet(device):
        pl.semaphore_signal(barrier, inc=1, device_id=device, device_id_type=MESH)

    each(1, half, lambda turn: greet({"rows": partner(n - 2 * turn)}))
    greet({"rows": partner(1)})
    each(1, n_feat, lambda step: greet(device_after(step)))

    for copy in small:
        copy.wait()
    leaf, grad, hess = (ref[...].astype(jnp.float32) for ref in (leaf_ref, grad_ref, hess_ref))
    spare = jnp.zeros((meta_src.shape[1] - 3 * share, LANES), jnp.float32)
    for part in range(n_feat):
        span = slice(part * share, (part + 1) * share)
        meta_src[part] = jnp.concatenate([leaf[span], grad[span], hess[span], spare], axis=0).astype(jnp.bfloat16)
    for piece in range(pieces):
        fetch(piece).wait()
        for tile in range(piece * piece_rows // LANES, (piece + 1) * piece_rows // LANES):
            lanes = slice(tile * LANES, (tile + 1) * LANES)
            turned = raw[lanes].astype(jnp.float32).astype(jnp.bfloat16).T
            bins_src[:, :, lanes] = turned.reshape(n, own, LANES)

    own_bins = pltpu.make_async_copy(bins_src.at[me], columns.at[me], own_sems.at[0])
    own_meta = pltpu.make_async_copy(meta_src, metas.at[:, me % 2, me // 2], own_sems.at[1])
    own_bins.start()
    own_meta.start()
    pl.semaphore_wait(barrier, half + n_feat - 1)

    def bin_copy(step, landed):
        other = partner(step)
        return pltpu.make_async_remote_copy(
            src_ref=bins_src.at[other], dst_ref=columns.at[other if landed else me], send_sem=bin_send,
            recv_sem=bin_recv.at[step], device_id={"rows": other}, device_id_type=MESH)

    def late_copy(step, part, landed):
        other = partner(step)
        some = pl.ds(part * (rows // 2), rows // 2)
        return pltpu.make_async_remote_copy(
            src_ref=bins_src.at[other, :, some], dst_ref=columns.at[other if landed else me, :, some],
            send_sem=bin_send, recv_sem=bin_recv.at[step + 2 * part],
            device_id={"rows": other}, device_id_type=MESH)

    def use_step(place):
        later = place - 2
        turns = jnp.where(later % 2 == 0, 2 + later // 2, half + later // 2)
        near_left = 2 + later - quarter
        step = jnp.where(later < 2 * quarter, turns, jnp.where(place < half + quarter, near_left, place))
        return jnp.where(later < 0, place, step)

    def send_step(place):
        turns = 1 + place // 2 + (place % 2) * (half - 1)
        return jnp.where(place < half, turns, jnp.where(place < half + quarter - 1, 1 + place - quarter, place + 1))

    def near_meta(step, landed):
        other = partner(step)
        row = other if landed else me
        return pltpu.make_async_remote_copy(
            src_ref=meta_src, dst_ref=metas.at[:, row % 2, row // 2], send_sem=near_send,
            recv_sem=near_recv.at[step], device_id={"rows": other}, device_id_type=MESH)

    def far_meta(step):
        return pltpu.make_async_remote_copy(
            src_ref=meta_src.at[me_feat], dst_ref=metas.at[me_feat, side, me // 2], send_sem=far_send,
            recv_sem=far_recv, device_id={"rows": partner(step)}, device_id_type=MESH)

    far_rows = metas.at[0, 0, pl.ds(0, quarter)]
    near_rows = metas.at[:, 0, pl.ds(0, half - 1)]
    sent_blocks = columns.at[pl.ds(0, n - 1)]
    reports = landing.at[pl.ds(1, everyone - 1)]

    def swap_meta(step):
        far = metas.at[me_feat, side, pl.ds(across, quarter)]
        return pltpu.make_async_remote_copy(
            src_ref=far, dst_ref=far, send_sem=swap_send, recv_sem=swap_recv,
            device_id={"rows": partner(1) if step >= n_feat else me, "feat": lax.rem(me_feat + step % n_feat, n_feat)},
            device_id_type=MESH)

    def await_swaps(sem):
        pltpu.make_async_copy(tally, tally, sem).wait()

    pl.semaphore_signal(side_in, inc=1, device_id={"rows": partner(1)}, device_id_type=MESH)
    each(quarter, half, lambda turn: far_meta(2 * turn).start())
    near_meta(1, False).start()
    each(1, quarter, lambda turn: near_meta(2 * turn, False).start())
    late = [(step, part) for part in range(2) for step in (n - 2, n - 1)]
    each(0, 2, lambda place: bin_copy(send_step(place), False).start())

    def send_rest():
        pl.semaphore_wait(side_in, 1)
        each(1, quarter, lambda turn: near_meta(2 * turn + 1, False).start())
        each(2, n - 3, lambda place: bin_copy(send_step(place), False).start())
        for step, part in sorted(late):
            late_copy(step, part, False).start()

    landing[0] = jnp.full((1, LANES), -jnp.inf, jnp.float32)
    own_bins.wait()
    own_meta.wait()

    pairs = -(-own // 2)

    def compute(*sums):
        for total in sums:
            pltpu.matmul_pop(total)
        send_rest()
        lax.fori_loop(0, n - 2, functools.partial(one_shard, sums), 0)
        for step, part in sorted(late):
            late_copy(step, part, True).wait_recv()
            add_rows(sums, partner(step), part * (tiles // 2), (part + 1) * (tiles // 2))
        for refs, sem in ((sent_blocks, bin_send), (near_rows, near_send), (far_rows, far_send)):
            pltpu.make_async_copy(refs, refs, sem).wait()
        await_swaps(swap_send)
        largest = jnp.full((LEAVES, HALF), -jnp.inf, jnp.float32)
        for pair in range(pairs):
            largest = gains(pair, pltpu.matmul_pop(sums[pair]), largest)
        largest = jnp.broadcast_to(jnp.max(largest, axis=1, keepdims=True), (LEAVES, LANES))
        on_lane = (lax.broadcasted_iota(jnp.int32, (LEAVES, LANES), 0)
                   == lax.broadcasted_iota(jnp.int32, (LEAVES, LANES), 1))
        top[...] = jnp.max(jnp.where(on_lane, largest, -jnp.inf), axis=0, keepdims=True)

    def one_shard(sums, place, carry):
        step = use_step(place)
        origin = partner(step)

        @pl.when(place == 2)
        def swap():
            pltpu.make_async_copy(far_rows, far_rows, far_recv).wait()
            for other in range(1, 2 * n_feat):
                swap_meta(other).start()

        @pl.when(jnp.logical_and(step > 0, step < half))
        def near_arrived():
            near_meta(step, True).wait_recv()

        @pl.when(place == 3)
        def swapped():
            await_swaps(swap_recv)

        @pl.when(step > 0)
        def arrived():
            bin_copy(step, True).wait_recv()

        add_rows(sums, origin, 0, tiles)
        return carry

    def add_rows(sums, origin, first_tile, last_tile):
        table = metas[:, origin % 2, origin // 2].astype(jnp.float32)
        leaf_of = lax.broadcasted_iota(jnp.int32, (LEAVES, LANES), 0).astype(jnp.float32)
        for tile in range(first_tile, last_tile):
            piece, row = tile // share, tile % share
            member = jnp.broadcast_to(table[piece, row:row + 1], (LEAVES, LANES)) == leaf_of
            for part in (0, 1):
                first = (1 + part) * share + row
                value = jnp.broadcast_to(table[piece, first:first + 1], (LEAVES, LANES))
                weights[part * LEAVES:(part + 1) * LEAVES, tile * LANES:(tile + 1) * LANES] = (
                    jnp.where(member, value, 0.0).astype(jnp.bfloat16))

        begin = first_tile * LANES
        block = columns[origin, :, begin:last_tile * LANES]
        low = jnp.where(block >= HALF, block - HALF, block)
        level = lax.broadcasted_iota(jnp.int32, (HALF, DEPTH), 0).astype(jnp.bfloat16)
        zero = jnp.zeros((), jnp.bfloat16)
        hit, miss = (jnp.full((HALF, DEPTH), value, jnp.float8_e4m3fn) for value in (1, 0))

        def step_of(feature, lanes):
            reached = jnp.broadcast_to(low[feature:feature + 1, lanes], (HALF, DEPTH)) <= level
            return jnp.where(reached, hit, miss)

        def upper_of(feature, lanes, table_rows):
            upper = jnp.broadcast_to(block[feature:feature + 1, lanes], (2 * LEAVES, DEPTH)) >= HALF
            return jnp.where(upper, table_rows, zero)

        for first in range(0, pairs, 2):
            for chunk in range(block.shape[1] // DEPTH):
                lanes = slice(chunk * DEPTH, (chunk + 1) * DEPTH)
                table_rows = weights[:, begin + chunk * DEPTH:begin + (chunk + 1) * DEPTH]
                for pair in range(first, min(first + 2, pairs)):
                    features = (2 * pair, min(2 * pair + 1, own - 1))
                    steps = jnp.concatenate([step_of(feature, lanes) for feature in features], axis=0)
                    turned = (chunk + pair) % 3 != 0
                    pltpu.matmul_push_rhs(
                        steps.T if turned else steps,
                        staging_register=chunk % 2, mxu_index=pair % 2, transpose=not turned)
                    pltpu.matmul_acc_lhs(
                        sums[pair],
                        jnp.concatenate([table_rows] + [upper_of(feature, lanes, table_rows) for feature in features], axis=0),
                        load_staged_rhs=chunk % 2)

    def gains(pair, part, largest):
        for place in range(2):
            feature = 2 * pair + place
            if feature == own:
                break
            lanes = slice(place * HALF, (place + 1) * HALF)
            both = part[:2 * LEAVES, lanes]
            upper = part[(1 + place) * 2 * LEAVES:(2 + place) * 2 * LEAVES, lanes]
            total = both[:, HALF - 1:]
            lower, beyond = both - upper, upper[:, HALF - 1:] - upper
            total_grad, total_hess = total[:LEAVES], total[LEAVES:]
            whole = total_grad * total_grad / (total_hess + reg_lambda)
            for side, left, right in ((0, lower, total - lower), (1, total - beyond, beyond)):
                left_grad, left_hess = left[:LEAVES], left[LEAVES:]
                right_grad, right_hess = right[:LEAVES], right[LEAVES:]
                gain = 0.5 * (left_grad * left_grad / (left_hess + reg_lambda)
                              + right_grad * right_grad / (right_hess + reg_lambda) - whole)
                gain_ref[feature, :, side * HALF:(side + 1) * HALF] = gain
                largest = jnp.maximum(largest, gain)
        return largest

    pl.run_scoped(compute, *[pltpu.ACC(pair % 2)((6 * LEAVES, 2 * HALF), jnp.float32) for pair in range(pairs)])

    def report(place):
        step = everyone - place
        return pltpu.make_async_remote_copy(
            src_ref=top, dst_ref=landing.at[step], send_sem=top_send,
            recv_sem=top_recv, device_id=device_after(step), device_id_type=MESH)

    each(1, everyone, lambda place: report(place).start())
    pltpu.make_async_copy(reports, reports, top_recv).wait()
    best = jnp.maximum(top[...], jnp.max(landing[...], axis=0))
    pltpu.make_async_copy(reports, reports, top_send).wait()
    best_ref[...] = best[:, :LEAVES]


def body(bin_index, leaf_ids, gradients, hessians):
    n, n_feat = lax.axis_size("rows"), lax.axis_size("feat")
    rows, local_features = bin_index.shape
    own = local_features // n
    tiles = rows // LANES
    pieces = 2
    everyone = n * n_feat
    half = n // 2
    meta_rows = -(-3 * (tiles // n_feat) // 16) * 16
    vmem = pl.BlockSpec(memory_space=pltpu.VMEM)
    dma = pltpu.SemaphoreType.DMA
    gain, best = pl.pallas_call(
        functools.partial(kernel, n, n_feat),
        out_shape=(pltpu.VMEM((own, LEAVES, BINS), jnp.float32),
                   pltpu.VMEM((1, LEAVES), jnp.float32)),
        in_specs=[pl.BlockSpec(memory_space=pl.ANY)] * 4,
        out_specs=(vmem, vmem),
        scratch_shapes=[
            pltpu.VMEM((tiles, LANES), jnp.int32),
            pltpu.VMEM((tiles, LANES), jnp.bfloat16),
            pltpu.VMEM((tiles, LANES), jnp.bfloat16),
            dma((3,)),
            pltpu.VMEM((rows, local_features), jnp.int32),
            pltpu.VMEM((n, own, rows), jnp.bfloat16),
            pltpu.VMEM((n_feat, meta_rows, LANES), jnp.bfloat16),
            pltpu.VMEM((n, own, rows), jnp.bfloat16),
            pltpu.VMEM((n_feat, 2, half, meta_rows, LANES), jnp.bfloat16),
            pltpu.VMEM((2 * LEAVES, rows), jnp.bfloat16),
            pltpu.VMEM((1, LANES), jnp.float32),
            pltpu.VMEM((everyone, 1, LANES), jnp.float32),
            dma((pieces,)), dma, dma((n + 2,)), dma, dma((half,)), dma, dma, dma, dma, dma((2,)), dma, dma, pltpu.SemaphoreType.REGULAR,
            pltpu.VMEM((2 * n_feat - 1, n // 4, meta_rows, LANES), jnp.bfloat16),
        ],
        compiler_params=pltpu.CompilerParams(
            collective_id=0, has_side_effects=True, vmem_limit_bytes=60 * 1024 * 1024),
    )(bin_index, leaf_ids.reshape(tiles, LANES), gradients.reshape(tiles, LANES), hessians.reshape(tiles, LANES))
    return gain[None], best.reshape(LEAVES)


def solution(mesh):
    placed = (P("rows", "feat"), P("rows"), P("rows"), P("rows"))
    return jax.shard_map(
        body,
        mesh=mesh,
        in_specs=placed,
        out_specs=(P("feat", "rows", None, None), P()),
        check_vma=False,
    )
```

```python
import functools

import jax
import jax.numpy as jnp
from jax import lax
from jax.experimental import pallas as pl
from jax.experimental.pallas import tpu as pltpu
from jax.sharding import PartitionSpec as P

BINS = 256
LEAVES = 16
LANES = 128
HALF = BINS // 2
DEPTH = 256
MESH = pl.DeviceIdType.MESH

reg_lambda = 1.0


def kernel(n, n_feat, bins_hbm, leaf_hbm, grad_hbm, hess_hbm, gain_ref, best_ref,
           leaf_ref, grad_ref, hess_ref, small_sems, raw, bins_src, meta_src, columns, metas, weights, top, landing,
           raw_sems, bin_send, bin_recv, near_send, near_recv, far_send, far_recv, swap_send, swap_recv, own_sems,
           top_send, top_recv, side_in, tally):
    me, me_feat = lax.axis_index("rows"), lax.axis_index("feat")
    everyone = n * n_feat
    me_all = me * n_feat + me_feat
    own, rows = bins_src.shape[1], bins_src.shape[2]
    tiles = rows // LANES
    share = tiles // n_feat
    half, quarter = n // 2, n // 4
    side, across = me % 2, (1 - me // half) * quarter
    pieces = raw_sems.shape[0]
    piece_rows = rows // pieces

    def fetch(piece, first=0, count=piece_rows):
        span = pl.ds(piece * piece_rows + first, count)
        return pltpu.make_async_copy(bins_hbm.at[span], raw.at[span], raw_sems.at[piece])

    small = [pltpu.make_async_copy(source, target, small_sems.at[place]) for place, (source, target) in enumerate(
        ((leaf_hbm, leaf_ref), (grad_hbm, grad_ref), (hess_hbm, hess_ref)))]
    for copy in small:
        copy.start()
    for piece in range(pieces):
        for first in range(0, piece_rows, 2 * LANES):
            fetch(piece, first, 2 * LANES).start()

    def partner(step):
        other, bit = 0, 1
        while bit < n:
            other += lax.rem(me // bit + step // bit, 2) * bit
            bit *= 2
        return other

    def device_after(step):
        return {"rows": partner(step // n_feat), "feat": lax.rem(me_feat + lax.rem(step, n_feat), n_feat)}

    barrier = pltpu.get_barrier_semaphore()

    def each(first, last, act):
        def run(step, carry):
            act(step)
            return carry
        lax.fori_loop(first, last, run, 0, unroll=everyone <= 64)

    def greet(device):
        pl.semaphore_signal(barrier, inc=1, device_id=device, device_id_type=MESH)

    each(1, half, lambda turn: greet({"rows": partner(n - 2 * turn)}))
    greet({"rows": partner(1)})
    each(1, n_feat, lambda step: greet(device_after(step)))

    for copy in small:
        copy.wait()
    leaf, grad, hess = (ref[...].astype(jnp.float32) for ref in (leaf_ref, grad_ref, hess_ref))
    spare = jnp.zeros((meta_src.shape[1] - 3 * share, LANES), jnp.float32)
    for part in range(n_feat):
        span = slice(part * share, (part + 1) * share)
        meta_src[part] = jnp.concatenate([leaf[span], grad[span], hess[span], spare], axis=0).astype(jnp.bfloat16)
    for piece in range(pieces):
        fetch(piece).wait()
        for tile in range(piece * piece_rows // LANES, (piece + 1) * piece_rows // LANES):
            lanes = slice(tile * LANES, (tile + 1) * LANES)
            turned = raw[lanes].astype(jnp.float32).astype(jnp.bfloat16).T
            bins_src[:, :, lanes] = turned.reshape(n, own, LANES)

    own_bins = pltpu.make_async_copy(bins_src.at[me], columns.at[me], own_sems.at[0])
    own_meta = pltpu.make_async_copy(meta_src, metas.at[:, me % 2, me // 2], own_sems.at[1])
    own_bins.start()
    own_meta.start()
    pl.semaphore_wait(barrier, half + n_feat - 1)

    def bin_copy(step, landed):
        other = partner(step)
        return pltpu.make_async_remote_copy(
            src_ref=bins_src.at[other], dst_ref=columns.at[other if landed else me], send_sem=bin_send,
            recv_sem=bin_recv.at[step], device_id={"rows": other}, device_id_type=MESH)

    def late_copy(step, part, landed):
        other = partner(step)
        some = pl.ds(part * (rows // 2), rows // 2)
        return pltpu.make_async_remote_copy(
            src_ref=bins_src.at[other, :, some], dst_ref=columns.at[other if landed else me, :, some],
            send_sem=bin_send, recv_sem=bin_recv.at[step + 2 * part],
            device_id={"rows": other}, device_id_type=MESH)

    def use_step(place):
        later = place - 2
        turns = jnp.where(later % 2 == 0, 2 + later // 2, half + later // 2)
        near_left = 2 + later - quarter
        step = jnp.where(later < 2 * quarter, turns, jnp.where(place < half + quarter, near_left, place))
        return jnp.where(later < 0, place, step)

    def send_step(place):
        turns = 1 + place // 2 + (place % 2) * (half - 1)
        return jnp.where(place < half, turns, jnp.where(place < half + quarter - 1, 1 + place - quarter, place + 1))

    def near_meta(step, landed):
        other = partner(step)
        row = other if landed else me
        return pltpu.make_async_remote_copy(
            src_ref=meta_src, dst_ref=metas.at[:, row % 2, row // 2], send_sem=near_send,
            recv_sem=near_recv.at[step], device_id={"rows": other}, device_id_type=MESH)

    def far_meta(step):
        return pltpu.make_async_remote_copy(
            src_ref=meta_src.at[me_feat], dst_ref=metas.at[me_feat, side, me // 2], send_sem=far_send,
            recv_sem=far_recv, device_id={"rows": partner(step)}, device_id_type=MESH)

    far_rows = metas.at[0, 0, pl.ds(0, quarter)]
    near_rows = metas.at[:, 0, pl.ds(0, half - 1)]
    sent_blocks = columns.at[pl.ds(0, n - 1)]
    reports = landing.at[pl.ds(1, everyone - 1)]

    def swap_meta(step):
        far = metas.at[me_feat, side, pl.ds(across, quarter)]
        return pltpu.make_async_remote_copy(
            src_ref=far, dst_ref=far, send_sem=swap_send, recv_sem=swap_recv,
            device_id={"rows": partner(1) if step >= n_feat else me, "feat": lax.rem(me_feat + step % n_feat, n_feat)},
            device_id_type=MESH)

    def await_swaps(sem):
        pltpu.make_async_copy(tally, tally, sem).wait()

    pl.semaphore_signal(side_in, inc=1, device_id={"rows": partner(1)}, device_id_type=MESH)
    each(quarter, half, lambda turn: far_meta(2 * turn).start())
    near_meta(1, False).start()
    each(1, quarter, lambda turn: near_meta(2 * turn, False).start())
    late = [(step, part) for part in range(2) for step in (n - 2, n - 1)]
    each(0, 3, lambda place: bin_copy(send_step(place), False).start())

    def send_rest():
        pl.semaphore_wait(side_in, 1)
        each(1, quarter, lambda turn: near_meta(2 * turn + 1, False).start())
        each(3, n - 3, lambda place: bin_copy(send_step(place), False).start())
        for step, part in sorted(late):
            late_copy(step, part, False).start()

    landing[0] = jnp.full((1, LANES), -jnp.inf, jnp.float32)
    own_bins.wait()
    own_meta.wait()

    pairs = -(-own // 2)

    def compute(*sums):
        for total in sums:
            pltpu.matmul_pop(total)
        send_rest()
        lax.fori_loop(0, n - 2, functools.partial(one_shard, sums), 0)
        for step, part in sorted(late):
            late_copy(step, part, True).wait_recv()
            add_rows(sums, partner(step), part * (tiles // 2), (part + 1) * (tiles // 2))
        for refs, sem in ((sent_blocks, bin_send), (near_rows, near_send), (far_rows, far_send)):
            pltpu.make_async_copy(refs, refs, sem).wait()
        await_swaps(swap_send)
        largest = jnp.full((LEAVES, HALF), -jnp.inf, jnp.float32)
        for pair in range(pairs):
            largest = gains(pair, pltpu.matmul_pop(sums[pair]), largest)
        largest = jnp.broadcast_to(jnp.max(largest, axis=1, keepdims=True), (LEAVES, LANES))
        on_lane = (lax.broadcasted_iota(jnp.int32, (LEAVES, LANES), 0)
                   == lax.broadcasted_iota(jnp.int32, (LEAVES, LANES), 1))
        top[...] = jnp.max(jnp.where(on_lane, largest, -jnp.inf), axis=0, keepdims=True)

    def one_shard(sums, place, carry):
        step = use_step(place)
        origin = partner(step)

        @pl.when(place == 2)
        def swap():
            pltpu.make_async_copy(far_rows, far_rows, far_recv).wait()
            for other in range(1, 2 * n_feat):
                swap_meta(other).start()

        @pl.when(jnp.logical_and(step > 0, step < half))
        def near_arrived():
            near_meta(step, True).wait_recv()

        @pl.when(place == 3)
        def swapped():
            await_swaps(swap_recv)

        @pl.when(step > 0)
        def arrived():
            bin_copy(step, True).wait_recv()

        add_rows(sums, origin, 0, tiles)
        return carry

    def add_rows(sums, origin, first_tile, last_tile):
        table = metas[:, origin % 2, origin // 2].astype(jnp.float32)
        leaf_of = lax.broadcasted_iota(jnp.int32, (LEAVES, LANES), 0).astype(jnp.float32)
        for tile in range(first_tile, last_tile):
            piece, row = tile // share, tile % share
            member = jnp.broadcast_to(table[piece, row:row + 1], (LEAVES, LANES)) == leaf_of
            for part in (0, 1):
                first = (1 + part) * share + row
                value = jnp.broadcast_to(table[piece, first:first + 1], (LEAVES, LANES))
                weights[part * LEAVES:(part + 1) * LEAVES, tile * LANES:(tile + 1) * LANES] = (
                    jnp.where(member, value, 0.0).astype(jnp.bfloat16))

        begin = first_tile * LANES
        block = columns[origin, :, begin:last_tile * LANES]
        low = jnp.where(block >= HALF, block - HALF, block)
        level = lax.broadcasted_iota(jnp.int32, (HALF, DEPTH), 0).astype(jnp.bfloat16)
        zero = jnp.zeros((), jnp.bfloat16)
        hit, miss = (jnp.full((HALF, DEPTH), value, jnp.float8_e4m3fn) for value in (1, 0))

        def step_of(feature, lanes):
            reached = jnp.broadcast_to(low[feature:feature + 1, lanes], (HALF, DEPTH)) <= level
            return jnp.where(reached, hit, miss)

        def upper_of(feature, lanes, table_rows):
            upper = jnp.broadcast_to(block[feature:feature + 1, lanes], (2 * LEAVES, DEPTH)) >= HALF
            return jnp.where(upper, table_rows, zero)

        for first in range(0, pairs, 2):
            for chunk in range(block.shape[1] // DEPTH):
                lanes = slice(chunk * DEPTH, (chunk + 1) * DEPTH)
                table_rows = weights[:, begin + chunk * DEPTH:begin + (chunk + 1) * DEPTH]
                for pair in range(first, min(first + 2, pairs)):
                    features = (2 * pair, min(2 * pair + 1, own - 1))
                    steps = jnp.concatenate([step_of(feature, lanes) for feature in features], axis=0)
                    turned = (chunk + pair) % 3 != 0
                    pltpu.matmul_push_rhs(
                        steps.T if turned else steps,
                        staging_register=chunk % 2, mxu_index=pair % 2, transpose=not turned)
                    pltpu.matmul_acc_lhs(
                        sums[pair],
                        jnp.concatenate([table_rows] + [upper_of(feature, lanes, table_rows) for feature in features], axis=0),
                        load_staged_rhs=chunk % 2)

    def gains(pair, part, largest):
        for place in range(2):
            feature = 2 * pair + place
            if feature == own:
                break
            lanes = slice(place * HALF, (place + 1) * HALF)
            both = part[:2 * LEAVES, lanes]
            upper = part[(1 + place) * 2 * LEAVES:(2 + place) * 2 * LEAVES, lanes]
            total = both[:, HALF - 1:]
            lower, beyond = both - upper, upper[:, HALF - 1:] - upper
            total_grad, total_hess = total[:LEAVES], total[LEAVES:]
            whole = total_grad * total_grad / (total_hess + reg_lambda)
            for side, left, right in ((0, lower, total - lower), (1, total - beyond, beyond)):
                left_grad, left_hess = left[:LEAVES], left[LEAVES:]
                right_grad, right_hess = right[:LEAVES], right[LEAVES:]
                gain = 0.5 * (left_grad * left_grad / (left_hess + reg_lambda)
                              + right_grad * right_grad / (right_hess + reg_lambda) - whole)
                gain_ref[feature, :, side * HALF:(side + 1) * HALF] = gain
                largest = jnp.maximum(largest, gain)
        return largest

    pl.run_scoped(compute, *[pltpu.ACC(pair % 2)((6 * LEAVES, 2 * HALF), jnp.float32) for pair in range(pairs)])

    def report(place):
        step = everyone - place
        return pltpu.make_async_remote_copy(
            src_ref=top, dst_ref=landing.at[step], send_sem=top_send,
            recv_sem=top_recv, device_id=device_after(step), device_id_type=MESH)

    each(1, everyone, lambda place: report(place).start())
    pltpu.make_async_copy(reports, reports, top_recv).wait()
    best = jnp.maximum(top[...], jnp.max(landing[...], axis=0))
    pltpu.make_async_copy(reports, reports, top_send).wait()
    best_ref[...] = best[:, :LEAVES]


def body(bin_index, leaf_ids, gradients, hessians):
    n, n_feat = lax.axis_size("rows"), lax.axis_size("feat")
    rows, local_features = bin_index.shape
    own = local_features // n
    tiles = rows // LANES
    pieces = 2
    everyone = n * n_feat
    half = n // 2
    meta_rows = -(-3 * (tiles // n_feat) // 16) * 16
    vmem = pl.BlockSpec(memory_space=pltpu.VMEM)
    dma = pltpu.SemaphoreType.DMA
    gain, best = pl.pallas_call(
        functools.partial(kernel, n, n_feat),
        out_shape=(pltpu.VMEM((own, LEAVES, BINS), jnp.float32),
                   pltpu.VMEM((1, LEAVES), jnp.float32)),
        in_specs=[pl.BlockSpec(memory_space=pl.ANY)] * 4,
        out_specs=(vmem, vmem),
        scratch_shapes=[
            pltpu.VMEM((tiles, LANES), jnp.int32),
            pltpu.VMEM((tiles, LANES), jnp.bfloat16),
            pltpu.VMEM((tiles, LANES), jnp.bfloat16),
            dma((3,)),
            pltpu.VMEM((rows, local_features), jnp.int32),
            pltpu.VMEM((n, own, rows), jnp.bfloat16),
            pltpu.VMEM((n_feat, meta_rows, LANES), jnp.bfloat16),
            pltpu.VMEM((n, own, rows), jnp.bfloat16),
            pltpu.VMEM((n_feat, 2, half, meta_rows, LANES), jnp.bfloat16),
            pltpu.VMEM((2 * LEAVES, rows), jnp.bfloat16),
            pltpu.VMEM((1, LANES), jnp.float32),
            pltpu.VMEM((everyone, 1, LANES), jnp.float32),
            dma((pieces,)), dma, dma((n + 2,)), dma, dma((half,)), dma, dma, dma, dma, dma((2,)), dma, dma, pltpu.SemaphoreType.REGULAR,
            pltpu.VMEM((2 * n_feat - 1, n // 4, meta_rows, LANES), jnp.bfloat16),
        ],
        compiler_params=pltpu.CompilerParams(
            collective_id=0, has_side_effects=True, vmem_limit_bytes=60 * 1024 * 1024),
    )(bin_index, leaf_ids.reshape(tiles, LANES), gradients.reshape(tiles, LANES), hessians.reshape(tiles, LANES))
    return gain[None], best.reshape(LEAVES)


def solution(mesh):
    placed = (P("rows", "feat"), P("rows"), P("rows"), P("rows"))
    return jax.shard_map(
        body,
        mesh=mesh,
        in_specs=placed,
        out_specs=(P("feat", "rows", None, None), P()),
        check_vma=False,
    )
```
